32 devices in a mesh: grp: 4 (over y, core), head: 8 (over z, x).
Axes of the slice: x: 2, y: 2, z: 4, core: 2. Of those that a mesh axis runs over, the one named last changes fastest.
Arguments:
- hidden_in: bfloat16 [96, 4096], P('grp', 'head'), may hold values from -6 to 6
- attention_gain: float32 [4096], replicated, may hold values from 0.1 to 1.9
- w_query: bfloat16 [4096, 4096], P(None, 'head'), may hold values from -0.09375 to 0.09375
- w_key_value: bfloat16 [2, 4096, 4096], P(None, None, 'head'), as said below
- w_attention_out: bfloat16 [4096, 4096], P('head'), may hold values from -0.09375 to 0.09375
- past_cache: bfloat16 [2, 96, 32, 128, 128], P(None, 'grp', 'head'), may hold values from -2000 to 2000, as said below
- lengths: int32 [96], P('grp'), may hold values from 2 to 128, as said below
- mamba_gain: float32 [4096], replicated, may hold values from 0.1 to 1.9
- w_in: bfloat16 [2, 4096, 8192], P(None, None, 'head'), may hold values from -0.09375 to 0.09375
- filter_weight: float32 [4, 8192], P(None, 'head'), may hold values from -3 to 3
- filter_bias: float32 [8192], P('head'), may hold values from -1.8 to 1.8
- filter_state: float32 [96, 3, 8192], P('grp', None, 'head'), may hold values from -6 to 6
- w_select: bfloat16 [8192, 288], P('head'), may hold values from -0.0625 to 0.0625
- w_step: bfloat16 [256, 8192], P(None, 'head'), may hold values from -0.375 to 0.375
- step_bias: float32 [8192], P('head'), may hold values from -4 to -1
- log_rate: float32 [16, 8192], P(None, 'head'), may hold values from 0 to 2.77
- skip_gain: float32 [8192], P('head'), may hold values from 0.1 to 1.9
- scan_state: float32 [96, 16, 8192], P('grp', None, 'head'), may hold values from -6 to 6
- w_mamba_out: bfloat16 [8192, 4096], P('head'), may hold values from -0.0625 to 0.0625
- reward_terms: float32 [96, 128], P('grp', 'head'), may hold values from -60 to 60
- reward_mask: int32 [96, 128], P('grp', 'head'), may hold values 0 or 1
Outputs:
- hidden_out: bfloat16 [96, 4096], P('grp', 'head')
- new_key_value: bfloat16 [2, 96, 32, 128], P(None, 'grp', 'head')
- new_filter_state: float32 [96, 3, 8192], P('grp', None, 'head')
- new_scan_state: float32 [96, 16, 8192], P('grp', None, 'head')
- rewards: float32 [96], P('grp')
The draws below stay inside these ranges and needn't reach their ends.
Inputs may be any that keep to these rules, and one draw needn't show every extreme that they name: `w_key_value`: query heads that share a key-value head (4 of them in a row) hold equal copies. `past_cache`: query heads that share a key-value head (4 of them in a row) hold equal copies. `lengths`: the first sample's cache is full (128).
All inputs are finite; a program needn't handle non-finite values. No bound on the sum of `reward_mask` on one device may be relied on, other than what follows from the above.
Results may differ from the reference program's by a relative error of at most 0.012.
Values may be sent and summed in bfloat16 or wider, within the bound.
A program may use at most 128 MiB of HBM per device.

```python
import math
import jax
import jax.numpy as jnp
from jax import lax

D = 4096
HEADS = 32
KVH = 8
DH = 128
INNER = 8192
NSTATE = 16
CONV = 4
RANK = 256
CTX = 128
BATCH = 96


def draw_w_key_value(key, part):
    drawn = jax.random.normal(key, (2, D, KVH, DH), jnp.float32) * D ** (-0.5)
    copies = jnp.repeat(drawn, HEADS // KVH, axis=2)
    return copies.reshape(2, D, HEADS * DH).astype(jnp.bfloat16)


def draw_past_cache(key, part):
    base_key = jax.random.fold_in(key, 0)
    drawn = jnp.clip(jax.random.normal(base_key, (2, BATCH, KVH, CTX, DH), jnp.float32), -6.0, 6.0)
    return jnp.repeat(drawn, HEADS // KVH, axis=2).astype(jnp.bfloat16)


def draw_lengths(key, part):
    drawn = jax.random.randint(key, (BATCH,), 2, CTX + 1, dtype=jnp.int32)
    return drawn.at[0].set(CTX)


def draw_reward_terms(key, part):
    noise_key = jax.random.fold_in(key, 0)
    ramp = 1.0 + 2.0 * jnp.arange(CTX, dtype=jnp.float32) / (CTX - 1)
    noise = jnp.clip(jax.random.normal(noise_key, (BATCH, CTX), jnp.float32), -6.0, 6.0)
    return noise * ramp[None, :]


def plant(result, key, least, largest):
    shape = result.shape
    place = [jax.random.randint(jax.random.fold_in(key, axis), (), 0, shape[axis]) for axis in range(len(shape))]
    result = result.at[tuple(place)].set(least)
    longest = shape.index(max(shape))
    place[longest] = (place[longest] + 1) % shape[longest]
    return result.at[tuple(place)].set(largest)


def block_levels(own_key, extent, shards, low, high):
    def one(position, shards_of):
        steps = jax.random.uniform(jax.random.fold_in(jax.random.fold_in(own_key, 6), position), (shards_of,), jnp.float32, low / len(shards), high / len(shards))
        return jnp.repeat(jnp.exp(steps), extent[position] // shards_of).reshape((-1,) + (1,) * (len(extent) - position - 1))

    level = one(*shards[0])
    for cut in shards[1:]:
        level = level * one(*cut)
    return level


def bell_draw(stream_key, shape, width, limit, cuts=(), held_as=jnp.bfloat16):
    level = block_levels(stream_key, shape, cuts, -0.22, 0.18) if cuts else 1.0
    array = jax.random.normal(stream_key, shape, jnp.float32) * width * level
    return jnp.minimum(jnp.maximum(array, -limit), limit).astype(held_as)


def setup_inputs(seed: int = 0) -> dict:
    key_of = jax.random.split(jax.random.key(seed), 22)
    return {
        "hidden_in": bell_draw(key_of[0], (BATCH, D), 1.0, 6.0, ((0, 4), (1, 8))),
        "attention_gain": jnp.clip(1.0 + 0.18 * jax.random.normal(key_of[1], (D,), jnp.float32), 0.1, 1.9),
        "w_query": bell_draw(key_of[2], (D, HEADS * DH), D ** -0.5, 0.09375, ((1, 8),)),
        "w_key_value": draw_w_key_value(jax.random.fold_in(key_of[21], 71), 0),
        "w_attention_out": bell_draw(key_of[4], (HEADS * DH, D), (HEADS * DH) ** -0.5, 0.09375, ((0, 8),)),
        "past_cache": draw_past_cache(jax.random.fold_in(key_of[21], 71), 0),
        "lengths": draw_lengths(jax.random.fold_in(key_of[21], 71), 0),
        "mamba_gain": jnp.clip(1.0 + 0.18 * jax.random.normal(key_of[7], (D,), jnp.float32), 0.1, 1.9),
        "w_in": bell_draw(key_of[8], (2, D, INNER), D ** -0.5, 0.09375, ((2, 8),)),
        "filter_weight": bell_draw(key_of[9], (CONV, INNER), CONV ** -0.5, 3.0, ((1, 8),), jnp.float32),
        "filter_bias": bell_draw(key_of[10], (INNER,), 0.3, 1.8, ((0, 8),), jnp.float32),
        "filter_state": bell_draw(key_of[11], (BATCH, CONV - 1, INNER), 1.0, 6.0, ((0, 4), (2, 8)), jnp.float32),
        "w_select": bell_draw(key_of[12], (INNER, RANK + 2 * NSTATE), INNER ** -0.5, 0.0625, ((0, 8),)),
        "w_step": bell_draw(key_of[13], (RANK, INNER), RANK ** -0.5, 0.375, ((1, 8),)),
        "step_bias": jnp.clip(-4.0 + 3.0 * jax.random.uniform(key_of[14], (INNER,), jnp.float32) ** block_levels(key_of[14], (INNER,), ((0, 8),), -0.2, 0.2), -4.0, -1.0),
        "log_rate": jnp.clip(2.77 * jax.random.uniform(key_of[15], (NSTATE, INNER), jnp.float32) ** block_levels(key_of[15], (NSTATE, INNER), ((1, 8),), -0.2, 0.2), 0.0, 2.77),
        "skip_gain": jnp.clip(1.0 + 0.18 * jax.random.normal(key_of[16], (INNER,), jnp.float32), 0.1, 1.9),
        "scan_state": bell_draw(key_of[17], (BATCH, NSTATE, INNER), 1.0, 6.0, ((0, 4), (2, 8)), jnp.float32),
        "w_mamba_out": bell_draw(key_of[18], (INNER, D), INNER ** -0.5, 0.0625, ((0, 8),)),
        "reward_terms": draw_reward_terms(jax.random.fold_in(key_of[21], 71), 0),
        "reward_mask": plant((jax.random.randint(key_of[20], (BATCH, CTX), 0, 2) < 1).astype(jnp.int32), jax.random.fold_in(key_of[20], 1), 0, 1),
    }


EPS = 1e-06

def norm_rows(row_values, gain):
    values = row_values.astype(jnp.float32)
    factor = lax.rsqrt(lax.optimization_barrier(jnp.mean(values * values, axis=-1, keepdims=True)) + EPS)
    return (values * factor * gain).astype(jnp.bfloat16)

def attend_sample(query, cache, fresh, length):
    inv_root = 1.0 / math.sqrt(query.shape[-1])
    query_wide = query.astype(jnp.float32)
    scores = jnp.einsum('hd,htd->ht', query_wide, cache[0].astype(jnp.float32)) * inv_root
    positions = jnp.arange(cache.shape[2], dtype=jnp.int32)
    scores = jnp.where(positions[None, :] < length, scores, -jnp.inf)
    own_score = lax.optimization_barrier(jnp.sum(query_wide * fresh[0].astype(jnp.float32), axis=-1)) * inv_root
    row_max = jnp.maximum(lax.optimization_barrier(jnp.max(scores, axis=-1)), own_score)
    weights = jnp.exp(scores - row_max[:, None])
    own_weight = jnp.exp(own_score - row_max)
    denominator = lax.optimization_barrier(jnp.sum(weights, axis=-1)) + own_weight
    weights = (weights / denominator[:, None]).astype(jnp.bfloat16)
    own_weight = (own_weight / denominator).astype(jnp.bfloat16)
    blended = jnp.einsum('ht,htd->hd', weights.astype(jnp.float32), cache[1].astype(jnp.float32))
    blended = blended + own_weight.astype(jnp.float32)[:, None] * fresh[1].astype(jnp.float32)
    return blended.astype(jnp.bfloat16)

def reference(hidden_in, attention_gain, w_query, w_key_value, w_attention_out, past_cache, lengths, mamba_gain, w_in, filter_weight, filter_bias, filter_state, w_select, w_step, step_bias, log_rate, skip_gain, scan_state, w_mamba_out, reward_terms, reward_mask):
    normed = norm_rows(hidden_in, attention_gain)
    queries = jnp.dot(normed, w_query, preferred_element_type=jnp.float32).astype(jnp.bfloat16)
    queries = queries.reshape(BATCH, HEADS, DH)
    fresh_all = jnp.einsum('bd,kdc->kbc', normed.astype(jnp.float32), w_key_value.astype(jnp.float32))
    new_key_value = fresh_all.astype(jnp.bfloat16).reshape(2, BATCH, HEADS, DH)

    def one_sample(index):
        cache = lax.dynamic_index_in_dim(past_cache, index, 1, keepdims=False)
        fresh = lax.dynamic_index_in_dim(new_key_value, index, 1, keepdims=False)
        query = lax.dynamic_index_in_dim(queries, index, 0, keepdims=False)
        length = lax.dynamic_index_in_dim(lengths, index, 0, keepdims=False)
        return attend_sample(query, cache, fresh, length)
    attended = lax.map(one_sample, jnp.arange(BATCH, dtype=jnp.int32)).reshape(BATCH, HEADS * DH)
    head_terms = jnp.dot(attended, w_attention_out, preferred_element_type=jnp.float32)
    mixed = (hidden_in.astype(jnp.float32) + head_terms).astype(jnp.bfloat16)
    normed_two = norm_rows(mixed, mamba_gain)
    x_inner = jnp.dot(normed_two, w_in[0], preferred_element_type=jnp.float32)
    gate_part = jnp.dot(normed_two, w_in[1], preferred_element_type=jnp.float32)
    conv_sum = filter_bias + x_inner * filter_weight[CONV - 1]
    for tap_index in range(CONV - 1):
        conv_sum = conv_sum + filter_state[:, tap_index, :] * filter_weight[tap_index]
    conv_out = jax.nn.silu(conv_sum).astype(jnp.bfloat16)
    new_filter_state = jnp.concatenate([filter_state[:, 1:, :], x_inner[:, None, :]], axis=1)
    projected = jnp.dot(conv_out, w_select, preferred_element_type=jnp.float32)
    step_low = projected[:, :RANK].astype(jnp.bfloat16)
    b_input = projected[:, RANK:RANK + NSTATE]
    c_output = projected[:, RANK + NSTATE:]
    step_size = jax.nn.softplus(jnp.dot(step_low, w_step, preferred_element_type=jnp.float32) + step_bias)
    conv_value = conv_out.astype(jnp.float32)
    decay_rate = jnp.exp(-step_size[:, None, :] * jnp.exp(log_rate)[None, :, :])
    new_scan_state = decay_rate * scan_state + step_size[:, None, :] * b_input[:, :, None] * conv_value[:, None, :]
    scan_out = (lax.optimization_barrier(jnp.sum(c_output[:, :, None] * new_scan_state, axis=1)) + skip_gain * conv_value) * jax.nn.silu(gate_part)
    scan_out = scan_out.astype(jnp.bfloat16)
    hidden_out = (mixed.astype(jnp.float32) + jnp.dot(scan_out, w_mamba_out, preferred_element_type=jnp.float32)).astype(jnp.bfloat16)
    positions = jnp.arange(CTX, dtype=jnp.int32)
    live = (reward_mask == 1) & (positions[None, :] < lengths[:, None])
    rewards = lax.optimization_barrier(jnp.sum(jnp.where(live, reward_terms, 0.0), axis=1))
    return (hidden_out, new_key_value, new_filter_state, new_scan_state, rewards)
```

```python
import functools
import math

import jax
import jax.numpy as jnp
from jax import lax
from jax.experimental import pallas as pl
from jax.experimental.pallas import tpu as pltpu
from jax.sharding import PartitionSpec as P

EPS = 1e-06
SHARE = 4
LANES = 128
BF16 = jnp.bfloat16
F32 = jnp.float32
MESH = pl.DeviceIdType.MESH


def dot(a, b):
    return jnp.dot(a, b, preferred_element_type=F32)


def columns_of(index, width):
    return pl.ds(pl.multiple_of(index * width, width), width)


def tile_of(width):
    for tile in (512, 256):
        if width % tile == 0:
            return tile
    return width


def matmul(x_ref, w_ref, out_ref):
    width = w_ref.shape[1]
    tile = tile_of(width)

    def body(i, carry):
        cols = columns_of(i, tile)
        out_ref[:, cols] = dot(x_ref[...], w_ref[:, cols])
        return carry

    lax.fori_loop(0, width // tile, body, 0)


def norm_blocks(blocks, gain, out, width):
    n, samples = blocks.shape[0], blocks.shape[1]
    total = jnp.zeros((samples, 1), F32)
    for j in range(n):
        v = blocks[j].astype(F32)
        total = total + jnp.sum(v * v, axis=1, keepdims=True)
    factor = lax.rsqrt(total / (n * width) + EPS)
    for j in range(n):
        cols = slice(j * width, (j + 1) * width)
        out[:, cols] = (blocks[j].astype(F32) * factor * gain[:, cols]).astype(BF16)


def kernel(n, *refs):
    (
        hidden, again, wq, wkv, wao, cache, lengths, mgain, w_in, fw, fb, fs, wsel,
        wstep, sbias, lrate, skip, scan, wmo, rterm, rmask,
        hidden_out, nkv_out, nfs_out, scan_out, rew_out,
        full, v_again, v_wq, v_wkv, v_wao, v_cache, v_mgain, v_win, v_fw, v_fb, v_fs,
        v_wsel, v_wstep, v_sbias, v_lrate, v_skip, v_scan, v_wmo, v_rterm, v_rmask,
        normed, q3, kv3, len3, q2, kv2, send_a, recv_a, mixfull, xin, gate, nfs,
        sel_msg, conv, step, yrow, sout, send_b, recv_b, hout, bct, rew,
        load_sem, out_sem, send_sem, recv_sem,
    ) = refs
    me = lax.axis_index("head")
    samples, width = hidden.shape
    heads, head_size = cache.shape[2], cache.shape[4]
    groups = v_cache.shape[2]
    share = heads // groups
    rank = wstep.shape[0]
    states = lrate.shape[0]
    channels = lrate.shape[1]
    taps = fw.shape[0]

    loads = {}

    def load(name, src, dst, pieces=1):
        sem = load_sem.at[len(loads)]
        rows = src.shape[0]
        step_rows = rows // pieces
        for p in range(pieces):
            part = pl.ds(p * step_rows, step_rows)
            if pieces == 1:
                pltpu.make_async_copy(src, dst, sem).start()
            else:
                pltpu.make_async_copy(src.at[part], dst.at[part], sem).start()
        loads[name] = pltpu.make_async_copy(src, dst, sem)

    load("hidden", hidden, full.at[me])
    load("again", again, v_again)
    load("wq", wq, v_wq, 4)
    for g in range(groups):
        cols = pl.ds(g * share * head_size, head_size)
        mine = pl.ds(g * head_size, head_size)
        for i in range(2):
            load(("wkv", i, g), wkv.at[i, :, cols], v_wkv.at[i, :, mine], 2)
    for i in range(2):
        for g in range(groups):
            load(("cache", i, g), cache.at[i, :, g * share], v_cache.at[i, :, g])
    load("wao", wao, v_wao, 4)

    peers = [lax.rem(me + d, n) for d in range(1, n)]
    barrier = pltpu.get_barrier_semaphore()
    for peer in peers:
        pl.semaphore_signal(barrier, inc=1, device_id={"head": peer}, device_id_type=MESH)
    pl.semaphore_wait(barrier, n - 1)

    sent = []

    def send(stage, src, dst, d):
        copy = pltpu.make_async_remote_copy(
            src_ref=src,
            dst_ref=dst,
            send_sem=send_sem.at[stage, d],
            recv_sem=recv_sem.at[stage, me],
            device_id={"head": peers[d - 1]},
            device_id_type=MESH,
        )
        copy.start()
        sent.append(copy)

    def arrived(stage, dst_of, d):
        source = lax.rem(me + n - d, n)
        pltpu.make_async_remote_copy(
            src_ref=dst_of(source),
            dst_ref=dst_of(source),
            send_sem=send_sem.at[stage, d],
            recv_sem=recv_sem.at[stage, source],
            device_id={"head": peers[d - 1]},
            device_id_type=MESH,
        ).wait_recv()
        return source

    loads["hidden"].wait()
    for d in range(1, n):
        send(0, full.at[me], full.at[me], d)

    load("rterm", rterm, v_rterm)
    load("rmask", rmask, v_rmask)
    load("mgain", mgain, v_mgain)
    load("fw", fw, v_fw)
    load("fb", fb, v_fb)
    load("fs", fs, v_fs)
    load("win0", w_in.at[0], v_win.at[0], 8)
    load("wsel", wsel, v_wsel)
    load("win1", w_in.at[1], v_win.at[1], 8)
    load("wstep", wstep, v_wstep)
    load("sbias", sbias, v_sbias)
    load("lrate", lrate, v_lrate)
    load("skip", skip, v_skip)
    load("scan", scan, v_scan, 2 if samples % 2 == 0 else 1)
    load("wmo", wmo, v_wmo, 8)

    for b in range(samples):
        len3[b] = jnp.full((8, LANES), lengths[b], jnp.int32)
    loads["rterm"].wait()
    loads["rmask"].wait()
    cols_r = rterm.shape[1]
    len2 = len3[:, 0, :][:, :cols_r]
    place = me * cols_r + lax.broadcasted_iota(jnp.int32, (samples, cols_r), 1)
    live = (v_rmask[...] == 1) & (place < len2)
    part = jnp.sum(jnp.where(live, v_rterm[...], 0.0), axis=1, keepdims=True)
    high = part.astype(BF16).astype(F32)
    low = (part - high).astype(BF16).astype(F32)
    rest = part - high - low
    lane = lax.broadcasted_iota(jnp.int32, (samples, LANES), 1)
    pieces = jnp.where(lane == 0, high, jnp.where(lane == 1, low, jnp.where(lane == 2, rest, 0.0)))
    sel_msg[me] = jnp.zeros(sel_msg.shape[1:], BF16)
    sel_width = sel_msg.shape[2] - LANES
    sel_msg[me, :, sel_width:] = pieces.astype(BF16)

    loads["again"].wait()
    for d in range(1, n):
        arrived(0, lambda s: full.at[s], d)
    norm_blocks(full, v_again, normed, width)

    loads["wq"].wait()
    matmul(normed, v_wq, q2)
    for g in range(groups):
        for i in range(2):
            loads[("wkv", i, g)].wait()
    inv_root = 1.0 / math.sqrt(head_size)
    for i in range(2):
        fresh = dot(normed[...], v_wkv[i]).astype(BF16)
        for g in range(groups):
            one = fresh[:, g * head_size : (g + 1) * head_size]
            for s in range(share):
                h = g * share + s
                kv2[i, :, h * head_size : (h + 1) * head_size] = one
            wide = one.astype(F32)
            for s in range(8):
                kv3[i, g, :, s, :] = wide
    pltpu.make_async_copy(kv2, nkv_out, out_sem.at[0]).start()
    q3[...] = jnp.zeros_like(q3)
    for g in range(groups):
        for s in range(share):
            h = g * share + s
            q3[g, :, s, :] = q2[:, h * head_size : (h + 1) * head_size].astype(BF16).astype(F32)
    context = v_cache.shape[3]
    for g in range(groups):
        loads[("cache", 0, g)].wait()
        loads[("cache", 1, g)].wait()
        q = q3[g]
        scores = lax.dot_general(
            q.astype(BF16), v_cache[0, :, g], (((2,), (2,)), ((0,), (0,))),
            preferred_element_type=F32,
        ) * inv_root
        place3 = lax.broadcasted_iota(jnp.int32, (samples, 8, context), 2)
        scores = jnp.where(place3 < len3[...][:, :, :1], scores, -jnp.inf)
        own = jnp.sum(q * kv3[0, g], axis=2, keepdims=True) * inv_root
        top = jnp.maximum(jnp.max(scores, axis=2, keepdims=True), own)
        weights = jnp.exp(scores - top)
        own_w = jnp.exp(own - top)
        denom = jnp.sum(weights, axis=2, keepdims=True) + own_w
        weights = (weights / denom).astype(BF16)
        own_w = (own_w / denom).astype(BF16).astype(F32)
        blended = lax.dot_general(
            weights, v_cache[1, :, g], (((2,), (1,)), ((0,), (0,))),
            preferred_element_type=F32,
        )
        q3[g] = blended + own_w * kv3[1, g]
    attended = jnp.concatenate(
        [q3[g, :, s, :] for g in range(groups) for s in range(share)], axis=1
    ).astype(BF16)

    loads["wao"].wait()
    for d in range(1, n):
        send_a[d] = dot(attended, v_wao[:, columns_of(peers[d - 1], width)]).astype(BF16)
        send(1, send_a.at[d], recv_a.at[me], d)
    mixed = full[me].astype(F32) + dot(attended, v_wao[:, columns_of(me, width)])
    for d in range(1, n):
        source = arrived(1, lambda s: recv_a.at[s], d)
        mixed = mixed + recv_a[source].astype(F32)
    mixfull[me] = mixed.astype(BF16)
    for d in range(1, n):
        send(2, mixfull.at[me], mixfull.at[me], d)
    loads["mgain"].wait()
    loads["fw"].wait()
    loads["fb"].wait()
    loads["fs"].wait()
    loads["win0"].wait()
    loads["wsel"].wait()
    base = jnp.broadcast_to(v_fb[...], (samples, channels))
    for k in range(taps - 1):
        base = base + v_fs[:, k, :] * v_fw[k : k + 1, :]
    conv[...] = base
    for k in range(taps - 2):
        nfs[:, k, :] = v_fs[:, k + 1, :]
    for d in range(1, n):
        arrived(2, lambda s: mixfull.at[s], d)
    norm_blocks(mixfull, v_mgain, normed, width)

    matmul(normed, v_win.at[0], xin)
    x_inner = xin[...]
    conv_sum = conv[...] + x_inner * v_fw[taps - 1 : taps, :]
    conv_b = (conv_sum * jax.nn.sigmoid(conv_sum)).astype(BF16)
    conv[...] = conv_b.astype(F32)
    sel_msg[me, :, :rank] = dot(conv_b, v_wsel[:, :rank]).astype(BF16)
    sel_msg[me, :, rank : rank + 2 * states] = dot(conv_b, v_wsel[:, rank:]).astype(BF16)
    for d in range(1, n):
        send(3, sel_msg.at[me], sel_msg.at[me], d)
    nfs[:, taps - 2, :] = x_inner
    pltpu.make_async_copy(nfs, nfs_out, out_sem.at[1]).start()
    loads["win1"].wait()
    matmul(normed, v_win.at[1], gate)
    g_part = gate[...]
    gate[...] = g_part * jax.nn.sigmoid(g_part)
    for name in ("wstep", "sbias", "lrate", "skip", "scan"):
        loads[name].wait()
    rate = -jnp.exp(v_lrate[...])
    v_lrate[...] = rate
    for d in range(1, n):
        arrived(3, lambda s: sel_msg.at[s], d)
    projected = sel_msg[0].astype(F32)
    for j in range(1, n):
        projected = projected + sel_msg[j].astype(F32)
    step_low = projected[:, :rank].astype(BF16)
    raw = dot(step_low, v_wstep[...]) + v_sbias[...]
    step[...] = jnp.maximum(raw, 0.0) + jnp.log1p(jnp.exp(-jnp.abs(raw)))
    bct[...] = jnp.zeros_like(bct)
    bct[:samples, :] = projected[:, rank : rank + LANES]
    flipped = jnp.transpose(bct[...])
    bct[...] = flipped
    total = jnp.sum(projected[:, sel_width:], axis=1, keepdims=True)
    diagonal = lax.broadcasted_iota(jnp.int32, (samples, LANES), 0) == lane
    row = jnp.sum(jnp.where(diagonal, total, 0.0), axis=0, keepdims=True)
    rew[...] = row[:, :samples]

    for b in range(samples):
        now = step[b : b + 1, :]
        decay = jnp.exp(now * v_lrate[...])
        b_col = bct[:states, b : b + 1]
        c_col = bct[states : 2 * states, b : b + 1]
        state = decay * v_scan[b] + b_col * (now * conv[b : b + 1, :])
        v_scan[b] = state
        yrow[b : b + 1, :] = jnp.sum(c_col * state, axis=0, keepdims=True)
    pltpu.make_async_copy(v_scan, scan_out, out_sem.at[2]).start()
    sout[...] = ((yrow[...] + v_skip[...] * conv[...]) * gate[...]).astype(BF16)

    loads["wmo"].wait()
    for d in range(1, n):
        send_b[d] = dot(sout[...], v_wmo[:, columns_of(peers[d - 1], width)]).astype(BF16)
        send(4, send_b.at[d], recv_b.at[me], d)
    final = mixfull[me].astype(F32) + dot(sout[...], v_wmo[:, columns_of(me, width)])
    pltpu.make_async_copy(rew, rew_out, out_sem.at[3]).start()
    for d in range(1, n):
        source = arrived(4, lambda s: recv_b.at[s], d)
        final = final + recv_b[source].astype(F32)
    hout[...] = final.astype(BF16)
    pltpu.make_async_copy(hout, hidden_out, out_sem.at[4]).start()
    for copy in sent:
        copy.wait_send()
    for i, (src, dst) in enumerate(
        ((kv2, nkv_out), (nfs, nfs_out), (v_scan, scan_out), (rew, rew_out), (hout, hidden_out))
    ):
        pltpu.make_async_copy(src, dst, out_sem.at[i]).wait()


def local(n, *args):
    (
        hidden, again, wq, wkv, wao, cache, lengths, mgain, w_in, fw, fb, fs, wsel,
        wstep, sbias, lrate, skip, scan, wmo, rterm, rmask,
    ) = args
    samples, width = hidden.shape
    heads, context, head_size = cache.shape[2:]
    share = min(SHARE, heads)
    groups = heads // share
    model = wq.shape[0]
    states, channels = lrate.shape
    row = lambda a: a.reshape(1, a.shape[0])
    args = (
        hidden, row(again), wq, wkv, wao, cache, lengths, row(mgain), w_in, fw, row(fb), fs,
        wsel, wstep, row(sbias), lrate, row(skip), scan, wmo, rterm, rmask,
    )
    sel_pad = -(-wsel.shape[1] // LANES) * LANES + LANES
    same = lambda a: pltpu.VMEM(a.shape, a.dtype)
    scratch = [
        pltpu.VMEM((n, samples, width), BF16),
        same(args[1]),
        same(wq),
        pltpu.VMEM((2, model, groups * head_size), BF16),
        same(wao),
        pltpu.VMEM((2, samples, groups, context, head_size), BF16),
        same(args[7]),
        same(w_in),
        same(fw),
        same(args[10]),
        same(fs),
        same(wsel),
        same(wstep),
        same(args[14]),
        same(lrate),
        same(args[16]),
        same(scan),
        same(wmo),
        same(rterm),
        same(rmask),
        pltpu.VMEM((samples, model), BF16),
        pltpu.VMEM((groups, samples, 8, head_size), F32),
        pltpu.VMEM((2, groups, samples, 8, head_size), F32),
        pltpu.VMEM((samples, 8, LANES), jnp.int32),
        pltpu.VMEM((samples, heads * head_size), F32),
        pltpu.VMEM((2, samples, heads * head_size), BF16),
        pltpu.VMEM((n, samples, width), BF16),
        pltpu.VMEM((n, samples, width), BF16),
        pltpu.VMEM((n, samples, width), BF16),
        pltpu.VMEM((samples, channels), F32),
        pltpu.VMEM((samples, channels), F32),
        same(fs),
        pltpu.VMEM((n, samples, sel_pad), BF16),
        pltpu.VMEM((samples, channels), F32),
        pltpu.VMEM((samples, channels), F32),
        pltpu.VMEM((samples, channels), F32),
        pltpu.VMEM((samples, channels), BF16),
        pltpu.VMEM((n, samples, width), BF16),
        pltpu.VMEM((n, samples, width), BF16),
        pltpu.VMEM((samples, width), BF16),
        pltpu.VMEM((LANES, LANES), F32),
        pltpu.VMEM((1, samples), F32),
        pltpu.SemaphoreType.DMA((19 + 4 * groups,)),
        pltpu.SemaphoreType.DMA((5,)),
        pltpu.SemaphoreType.DMA((5, n)),
        pltpu.SemaphoreType.DMA((5, n)),
    ]
    in_specs = [pl.BlockSpec(memory_space=pl.ANY)] * len(args)
    in_specs[6] = pl.BlockSpec(memory_space=pltpu.SMEM)
    hidden_out, nkv, nfs, new_scan, rewards = pl.pallas_call(
        functools.partial(kernel, n),
        out_shape=(
            jax.ShapeDtypeStruct((samples, width), BF16),
            jax.ShapeDtypeStruct((2, samples, heads * head_size), BF16),
            jax.ShapeDtypeStruct(fs.shape, F32),
            jax.ShapeDtypeStruct(scan.shape, F32),
            jax.ShapeDtypeStruct((1, samples), F32),
        ),
        in_specs=in_specs,
        out_specs=[pl.BlockSpec(memory_space=pl.ANY)] * 5,
        scratch_shapes=scratch,
        compiler_params=pltpu.CompilerParams(
            collective_id=0, has_side_effects=True, vmem_limit_bytes=67043328
        ),
        name="decode_step",
    )(*args)
    return (
        hidden_out,
        nkv.reshape(2, samples, heads, head_size),
        nfs,
        new_scan,
        rewards.reshape(samples),
    )


def solution(mesh):
    placed = (
        P("grp", "head"),
        P(),
        P(None, "head"),
        P(None, None, "head"),
        P("head", None),
        P(None, "grp", "head", None, None),
        P("grp"),
        P(),
        P(None, None, "head"),
        P(None, "head"),
        P("head"),
        P("grp", None, "head"),
        P("head", None),
        P(None, "head"),
        P("head"),
        P(None, "head"),
        P("head"),
        P("grp", None, "head"),
        P("head", None),
        P("grp", "head"),
        P("grp", "head"),
    )
    return jax.shard_map(
        functools.partial(local, mesh.shape["head"]),
        mesh=mesh,
        in_specs=placed,
        out_specs=(
            P("grp", "head"),
            P(None, "grp", "head", None),
            P("grp", None, "head"),
            P("grp", None, "head"),
            P("grp"),
        ),
        check_vma=False,
    )
```

```python
import functools
import math

import jax
import jax.numpy as jnp
from jax import lax
from jax.experimental import pallas as pl
from jax.experimental.pallas import tpu as pltpu
from jax.sharding import PartitionSpec as P

EPS = 1e-06
SHARE = 4
LANES = 128
BF16 = jnp.bfloat16
F32 = jnp.float32
MESH = pl.DeviceIdType.MESH


def dot(a, b):
    return jnp.dot(a, b, preferred_element_type=F32)


def columns_of(index, width):
    return pl.ds(pl.multiple_of(index * width, width), width)


def tile_of(width):
    for tile in (512, 256):
        if width % tile == 0:
            return tile
    return width


def matmul(x_ref, w_ref, out_ref):
    width = w_ref.shape[1]
    tile = tile_of(width)

    def body(i, carry):
        cols = columns_of(i, tile)
        out_ref[:, cols] = dot(x_ref[...], w_ref[:, cols])
        return carry

    lax.fori_loop(0, width // tile, body, 0)


def norm_blocks(blocks, gain, out, width):
    n, samples = blocks.shape[0], blocks.shape[1]
    total = jnp.zeros((samples, 1), F32)
    for j in range(n):
        v = blocks[j].astype(F32)
        total = total + jnp.sum(v * v, axis=1, keepdims=True)
    factor = lax.rsqrt(total / (n * width) + EPS)
    for j in range(n):
        cols = slice(j * width, (j + 1) * width)
        out[:, cols] = (blocks[j].astype(F32) * factor * gain[:, cols]).astype(BF16)


def kernel(n, *refs):
    (
        hidden, again, wq, wkv, wao, cache, lengths, mgain, w_in, fw, fb, fs, wsel,
        wstep, sbias, lrate, skip, scan, wmo, rterm, rmask,
        hidden_out, nkv_out, nfs_out, scan_out, rew_out,
        full, v_again, v_wq, v_wkv, v_wao, v_cache, v_mgain, v_win, v_fw, v_fb, v_fs,
        v_wsel, v_wstep, v_sbias, v_lrate, v_skip, v_scan, v_wmo, v_rterm, v_rmask,
        normed, q3, kv3, len3, q2, kv2, send_a, recv_a, mixfull, xin, gate, nfs,
        sel_msg, conv, step, yrow, sout, send_b, recv_b, hout, bct, rew, pieces,
        load_sem, out_sem, send_sem, recv_sem,
    ) = refs
    me = lax.axis_index("head")
    samples, width = hidden.shape
    heads, head_size = cache.shape[2], cache.shape[4]
    groups = v_cache.shape[2]
    share = heads // groups
    rank = wstep.shape[0]
    states = lrate.shape[0]
    channels = lrate.shape[1]
    taps = fw.shape[0]

    loads = {}

    def load(name, src, dst, pieces=1):
        sem = load_sem.at[len(loads)]
        rows = src.shape[0]
        step_rows = rows // pieces
        for p in range(pieces):
            part = pl.ds(p * step_rows, step_rows)
            if pieces == 1:
                pltpu.make_async_copy(src, dst, sem).start()
            else:
                pltpu.make_async_copy(src.at[part], dst.at[part], sem).start()
        loads[name] = pltpu.make_async_copy(src, dst, sem)

    load("hidden", hidden, full.at[me])
    load("again", again, v_again)
    load("wq", wq, v_wq, 4)
    for g in range(groups):
        cols = pl.ds(g * share * head_size, head_size)
        mine = pl.ds(g * head_size, head_size)
        for i in range(2):
            load(("wkv", i, g), wkv.at[i, :, cols], v_wkv.at[i, :, mine], 2)
    for i in range(2):
        for g in range(groups):
            load(("cache", i, g), cache.at[i, :, g * share], v_cache.at[i, :, g])
    load("wao", wao, v_wao, 4)

    peers = [lax.rem(me + d, n) for d in range(1, n)]
    barrier = pltpu.get_barrier_semaphore()
    for peer in peers:
        pl.semaphore_signal(barrier, inc=1, device_id={"head": peer}, device_id_type=MESH)
    pl.semaphore_wait(barrier, n - 1)

    sent = []

    def send(stage, src, dst, d):
        copy = pltpu.make_async_remote_copy(
            src_ref=src,
            dst_ref=dst,
            send_sem=send_sem.at[stage, d],
            recv_sem=recv_sem.at[stage, me],
            device_id={"head": peers[d - 1]},
            device_id_type=MESH,
        )
        copy.start()
        sent.append(copy)

    def arrived(stage, dst_of, d):
        source = lax.rem(me + n - d, n)
        pltpu.make_async_remote_copy(
            src_ref=dst_of(source),
            dst_ref=dst_of(source),
            send_sem=send_sem.at[stage, d],
            recv_sem=recv_sem.at[stage, source],
            device_id={"head": peers[d - 1]},
            device_id_type=MESH,
        ).wait_recv()
        return source

    loads["hidden"].wait()
    for d in range(1, n):
        send(0, full.at[me], full.at[me], d)

    load("rterm", rterm, v_rterm)
    load("rmask", rmask, v_rmask)
    load("mgain", mgain, v_mgain)
    load("fw", fw, v_fw)
    load("fb", fb, v_fb)
    load("fs", fs, v_fs)
    load("win0", w_in.at[0], v_win.at[0], 8)
    load("wsel", wsel, v_wsel.at[pl.ds(0, wsel.shape[0])])
    load("win1", w_in.at[1], v_win.at[1], 8)
    load("wstep", wstep, v_wstep)
    load("sbias", sbias, v_sbias)
    load("lrate", lrate, v_lrate)
    load("skip", skip, v_skip)
    load("scan", scan, v_scan, 2 if samples % 2 == 0 else 1)
    load("wmo", wmo, v_wmo, 8)

    for b in range(samples):
        len3[b] = jnp.full((8, LANES), lengths[b], jnp.int32)
    loads["rterm"].wait()
    loads["rmask"].wait()
    count = rterm.shape[0]
    diagonal = lax.broadcasted_iota(jnp.int32, (samples, samples), 0) == lax.broadcasted_iota(
        jnp.int32, (samples, samples), 1
    )
    len_row = jnp.sum(jnp.where(diagonal, len3[:, 0, :][:, :samples], 0), axis=0, keepdims=True)
    place = me * count + lax.broadcasted_iota(jnp.int32, (count, samples), 0)
    live = (v_rmask[...] == 1) & (place < len_row)
    part_row = jnp.sum(jnp.where(live, v_rterm[...], 0.0), axis=0, keepdims=True)
    part = jnp.sum(jnp.where(diagonal, part_row, 0.0), axis=1, keepdims=True)
    high = part.astype(BF16).astype(F32)
    low = (part - high).astype(BF16).astype(F32)
    rest = part - high - low
    selected = wsel.shape[0]
    padded = sel_msg.shape[2]
    lane = lax.broadcasted_iota(jnp.int32, (samples, padded), 1) - selected
    pieces[...] = jnp.where(
        lane == 0, high, jnp.where(lane == 1, low, jnp.where(lane == 2, rest, 0.0))
    )
    v_wsel[selected:, :] = jnp.zeros((padded - selected, channels), BF16)

    loads["again"].wait()
    for d in range(1, n):
        arrived(0, lambda s: full.at[s], d)
    norm_blocks(full, v_again, normed, width)

    loads["wq"].wait()
    matmul(normed, v_wq, q2)
    for g in range(groups):
        for i in range(2):
            loads[("wkv", i, g)].wait()
    inv_root = 1.0 / math.sqrt(head_size)
    for i in range(2):
        fresh = dot(normed[...], v_wkv[i]).astype(BF16)
        for g in range(groups):
            one = fresh[:, g * head_size : (g + 1) * head_size]
            wide = one.astype(F32)
            for s in range(8):
                kv3[i, g, :, s, :] = wide
            kv2[i, :, g * share : (g + 1) * share, :] = kv3[i, g].astype(BF16)[:, :share, :]
    pltpu.make_async_copy(kv2, nkv_out, out_sem.at[0]).start()
    q3[...] = jnp.zeros_like(q3)
    for g in range(groups):
        for s in range(share):
            h = g * share + s
            q3[g, :, s, :] = q2[:, h * head_size : (h + 1) * head_size].astype(BF16).astype(F32)
    context = v_cache.shape[3]
    for g in range(groups):
        loads[("cache", 0, g)].wait()
        loads[("cache", 1, g)].wait()
        q = q3[g]
        scores = lax.dot_general(
            q.astype(BF16), v_cache[0, :, g], (((2,), (2,)), ((0,), (0,))),
            preferred_element_type=F32,
        ) * inv_root
        place3 = lax.broadcasted_iota(jnp.int32, (samples, 8, context), 2)
        scores = jnp.where(place3 < len3[...][:, :, :1], scores, -jnp.inf)
        own = jnp.sum(q * kv3[0, g], axis=2, keepdims=True) * inv_root
        top = jnp.maximum(jnp.max(scores, axis=2, keepdims=True), own)
        weights = jnp.exp(scores - top)
        own_w = jnp.exp(own - top)
        denom = jnp.sum(weights, axis=2, keepdims=True) + own_w
        weights = (weights / denom).astype(BF16)
        own_w = (own_w / denom).astype(BF16).astype(F32)
        blended = lax.dot_general(
            weights, v_cache[1, :, g], (((2,), (1,)), ((0,), (0,))),
            preferred_element_type=F32,
        )
        q3[g] = blended + own_w * kv3[1, g]
    attended = jnp.concatenate(
        [q3[g, :, s, :] for g in range(groups) for s in range(share)], axis=1
    ).astype(BF16)

    loads["wao"].wait()
    for d in range(1, n):
        send_a[d] = dot(attended, v_wao[:, columns_of(peers[d - 1], width)]).astype(BF16)
        send(1, send_a.at[d], recv_a.at[me], d)
    mixed = full[me].astype(F32) + dot(attended, v_wao[:, columns_of(me, width)])
    for d in range(1, n):
        source = arrived(1, lambda s: recv_a.at[s], d)
        mixed = mixed + recv_a[source].astype(F32)
    mixfull[me] = mixed.astype(BF16)
    for d in range(1, n):
        send(2, mixfull.at[me], mixfull.at[me], d)
    loads["mgain"].wait()
    loads["fw"].wait()
    loads["fb"].wait()
    loads["fs"].wait()
    loads["win0"].wait()
    loads["wsel"].wait()
    base = jnp.broadcast_to(v_fb[...], (samples, channels))
    for k in range(taps - 1):
        base = base + v_fs[k] * v_fw[k : k + 1, :]
    conv[...] = base
    for k in range(taps - 2):
        nfs[k] = v_fs[k + 1]
    for d in range(1, n):
        arrived(2, lambda s: mixfull.at[s], d)
    norm_blocks(mixfull, v_mgain, normed, width)

    matmul(normed, v_win.at[0], xin)
    x_inner = xin[...]
    conv_sum = conv[...] + x_inner * v_fw[taps - 1 : taps, :]
    conv_b = (conv_sum * jax.nn.sigmoid(conv_sum)).astype(BF16)
    conv[...] = conv_b.astype(F32)
    picked = lax.dot_general(
        conv_b, v_wsel[...], (((1,), (1,)), ((), ())), preferred_element_type=F32
    )
    sel_msg[me] = (picked + pieces[...]).astype(BF16)
    for d in range(1, n):
        send(3, sel_msg.at[me], sel_msg.at[me], d)
    nfs[taps - 2] = x_inner
    pltpu.make_async_copy(nfs, nfs_out, out_sem.at[1]).start()
    loads["win1"].wait()
    matmul(normed, v_win.at[1], gate)
    g_part = gate[...]
    gate[...] = g_part * jax.nn.sigmoid(g_part)
    for name in ("wstep", "sbias", "lrate", "skip", "scan"):
        loads[name].wait()
    rate = -jnp.exp(v_lrate[...])
    v_lrate[...] = rate
    for d in range(1, n):
        arrived(3, lambda s: sel_msg.at[s], d)
    projected = sel_msg[0].astype(F32)
    for j in range(1, n):
        projected = projected + sel_msg[j].astype(F32)
    step_low = projected[:, :rank].astype(BF16)
    raw = dot(step_low, v_wstep[...]) + v_sbias[...]
    step[...] = jnp.maximum(raw, 0.0) + jnp.log1p(jnp.exp(-jnp.abs(raw)))
    bct[...] = jnp.zeros_like(bct)
    bct[:samples, :] = projected[:, rank : rank + LANES]
    flipped = jnp.transpose(bct[...])
    bct[...] = flipped
    total = jnp.sum(jnp.where((lane >= 0) & (lane < 3), projected, 0.0), axis=1, keepdims=True)
    rew[...] = jnp.sum(jnp.where(diagonal, total, 0.0), axis=0, keepdims=True)

    for b in range(samples):
        now = step[b : b + 1, :]
        decay = jnp.exp(now * v_lrate[...])
        b_col = bct[:states, b : b + 1]
        c_col = bct[states : 2 * states, b : b + 1]
        state = decay * v_scan[b] + b_col * (now * conv[b : b + 1, :])
        v_scan[b] = state
        yrow[b : b + 1, :] = jnp.sum(c_col * state, axis=0, keepdims=True)
    pltpu.make_async_copy(v_scan, scan_out, out_sem.at[2]).start()
    sout[...] = ((yrow[...] + v_skip[...] * conv[...]) * gate[...]).astype(BF16)

    loads["wmo"].wait()
    for d in range(1, n):
        send_b[d] = dot(sout[...], v_wmo[:, columns_of(peers[d - 1], width)]).astype(BF16)
        send(4, send_b.at[d], recv_b.at[me], d)
    final = mixfull[me].astype(F32) + dot(sout[...], v_wmo[:, columns_of(me, width)])
    pltpu.make_async_copy(rew, rew_out, out_sem.at[3]).start()
    for d in range(1, n):
        source = arrived(4, lambda s: recv_b.at[s], d)
        final = final + recv_b[source].astype(F32)
    hout[...] = final.astype(BF16)
    pltpu.make_async_copy(hout, hidden_out, out_sem.at[4]).start()
    for copy in sent:
        copy.wait_send()
    for i, (src, dst) in enumerate(
        ((kv2, nkv_out), (nfs, nfs_out), (v_scan, scan_out), (rew, rew_out), (hout, hidden_out))
    ):
        pltpu.make_async_copy(src, dst, out_sem.at[i]).wait()


def hand_out_kernel(parts, *refs):
    count = len(parts)
    sources, targets = refs[:count], refs[count : 2 * count]
    held = refs[2 * count : 3 * count]
    in_sem, out_sem = refs[3 * count :]
    pieces = []
    for i, cuts in enumerate(parts):
        rows = sources[i].shape[0] // cuts
        for c in range(cuts):
            pieces.append((i, pl.ds(c * rows, rows)))
    copies = []
    for k, (i, part) in enumerate(pieces):
        arrive = pltpu.make_async_copy(sources[i].at[part], held[i].at[part], in_sem.at[k])
        leave = pltpu.make_async_copy(held[i].at[part], targets[i].at[part], out_sem.at[k])
        arrive.start()
        copies.append((arrive, leave))
    for arrive, leave in copies:
        arrive.wait()
        leave.start()
    for arrive, leave in copies:
        leave.wait()


def hand_out(results):
    parts = [1] * len(results)
    for cuts in (8, 4, 2):
        if results[3].shape[0] % cuts == 0:
            parts[3] = cuts
            break
    total = sum(parts)
    return pl.pallas_call(
        functools.partial(hand_out_kernel, parts),
        out_shape=tuple(jax.ShapeDtypeStruct(a.shape, a.dtype) for a in results),
        in_specs=[pl.BlockSpec(memory_space=pl.ANY)] * len(results),
        out_specs=[pl.BlockSpec(memory_space=pl.ANY)] * len(results),
        scratch_shapes=[pltpu.VMEM(a.shape, a.dtype) for a in results]
        + [pltpu.SemaphoreType.DMA((total,)), pltpu.SemaphoreType.DMA((total,))],
        name="hand_out",
    )(*results)


def local(n, *args):
    (
        hidden, again, wq, wkv, wao, cache, lengths, mgain, w_in, fw, fb, fs, wsel,
        wstep, sbias, lrate, skip, scan, wmo, rterm, rmask,
    ) = args
    samples, width = hidden.shape
    heads, context, head_size = cache.shape[2:]
    share = min(SHARE, heads)
    groups = heads // share
    model = wq.shape[0]
    states, channels = lrate.shape
    row = lambda a: a.reshape(1, a.shape[0])
    args = (
        hidden, row(again), wq, wkv, wao, cache, lengths, row(mgain), w_in, fw, row(fb),
        jnp.transpose(fs, (1, 0, 2)), wsel.T, wstep, row(sbias), lrate, row(skip), scan, wmo,
        rterm.T, rmask.T,
    )
    sel_pad = -(-(wsel.shape[1] + 3) // LANES) * LANES
    same = lambda a: pltpu.VMEM(a.shape, a.dtype)
    scratch = [
        pltpu.VMEM((n, samples, width), BF16),
        same(args[1]),
        same(wq),
        pltpu.VMEM((2, model, groups * head_size), BF16),
        same(wao),
        pltpu.VMEM((2, samples, groups, context, head_size), BF16),
        same(args[7]),
        same(w_in),
        same(fw),
        same(args[10]),
        same(args[11]),
        pltpu.VMEM((sel_pad, channels), BF16),
        same(wstep),
        same(args[14]),
        same(lrate),
        same(args[16]),
        same(scan),
        same(wmo),
        same(args[19]),
        same(args[20]),
        pltpu.VMEM((samples, model), BF16),
        pltpu.VMEM((groups, samples, 8, head_size), F32),
        pltpu.VMEM((2, groups, samples, 8, head_size), F32),
        pltpu.VMEM((samples, 8, LANES), jnp.int32),
        pltpu.VMEM((samples, heads * head_size), F32),
        pltpu.VMEM((2, samples, heads, head_size), BF16),
        pltpu.VMEM((n, samples, width), BF16),
        pltpu.VMEM((n, samples, width), BF16),
        pltpu.VMEM((n, samples, width), BF16),
        pltpu.VMEM((samples, channels), F32),
        pltpu.VMEM((samples, channels), F32),
        same(args[11]),
        pltpu.VMEM((n, samples, sel_pad), BF16),
        pltpu.VMEM((samples, channels), F32),
        pltpu.VMEM((samples, channels), F32),
        pltpu.VMEM((samples, channels), F32),
        pltpu.VMEM((samples, channels), BF16),
        pltpu.VMEM((n, samples, width), BF16),
        pltpu.VMEM((n, samples, width), BF16),
        pltpu.VMEM((samples, width), BF16),
        pltpu.VMEM((LANES, LANES), F32),
        pltpu.VMEM((1, samples), F32),
        pltpu.VMEM((samples, sel_pad), F32),
        pltpu.SemaphoreType.DMA((19 + 4 * groups,)),
        pltpu.SemaphoreType.DMA((5,)),
        pltpu.SemaphoreType.DMA((5, n)),
        pltpu.SemaphoreType.DMA((5, n)),
    ]
    in_specs = [pl.BlockSpec(memory_space=pl.ANY)] * len(args)
    in_specs[6] = pl.BlockSpec(memory_space=pltpu.SMEM)
    results = pl.pallas_call(
        functools.partial(kernel, n),
        out_shape=(
            jax.ShapeDtypeStruct((samples, width), BF16),
            jax.ShapeDtypeStruct((2, samples, heads, head_size), BF16),
            jax.ShapeDtypeStruct(args[11].shape, F32),
            jax.ShapeDtypeStruct(scan.shape, F32),
            jax.ShapeDtypeStruct((1, samples), F32),
        ),
        in_specs=in_specs,
        out_specs=[pl.BlockSpec(memory_space=pl.ANY)] * 5,
        scratch_shapes=scratch,
        compiler_params=pltpu.CompilerParams(
            collective_id=0, has_side_effects=True, vmem_limit_bytes=67043328
        ),
        name="decode_step",
    )(*args)
    hidden_out, nkv, nfs, new_scan, rewards = hand_out(results)
    return hidden_out, nkv, jnp.transpose(nfs, (1, 0, 2)), new_scan, rewards.reshape(samples)


def solution(mesh):
    placed = (
        P("grp", "head"),
        P(),
        P(None, "head"),
        P(None, None, "head"),
        P("head", None),
        P(None, "grp", "head", None, None),
        P("grp"),
        P(),
        P(None, None, "head"),
        P(None, "head"),
        P("head"),
        P("grp", None, "head"),
        P("head", None),
        P(None, "head"),
        P("head"),
        P(None, "head"),
        P("head"),
        P("grp", None, "head"),
        P("head", None),
        P("grp", "head"),
        P("grp", "head"),
    )
    return jax.shard_map(
        functools.partial(local, mesh.shape["head"]),
        mesh=mesh,
        in_specs=placed,
        out_specs=(
            P("grp", "head"),
            P(None, "grp", "head", None),
            P("grp", None, "head"),
            P("grp", None, "head"),
            P("grp"),
        ),
        check_vma=False,
    )
```
